128 devices in a mesh: dp: 8 (over z_lo, y), inner: 16 (over z_hi, x, core).
Axes of the slice: x: 4, y: 4, z: 4 (z_hi: 2, z_lo: 2; z = z_hi * 2 + z_lo), core: 2. Of those that a mesh axis runs over, the one named last changes fastest.
Arguments:
- queries: bfloat16 [128, 32, 128], P(('dp', 'inner'))
- labels: int32 [128], P(('dp', 'inner')), may hold values from 0 to 511
- pages: bfloat16 [512, 1024, 128], P(('dp', 'inner'))
Outputs:
- grad_queries: float32 [128, 32, 128], P(('dp', 'inner'))
- grad_pages: float32 [512, 1024, 128], P(('dp', 'inner'))
The draws below stay inside these ranges and needn't reach their ends.
All inputs are finite; a program needn't handle non-finite values.
Results may differ from the reference program's by a relative error of at most 0.0029.
Values may be sent and summed in bfloat16 or wider, within the bound.
A program may use at most 64 MiB of HBM per device.

```python
import jax
import jax.numpy as jnp
from jax import lax

D = 128
LQ = 32
LP = 1024
QUERIES = 128
PAGES = 512


def draw_pages(key, part):
    values = jax.random.normal(jax.random.fold_in(key, 11), (PAGES, LP, D), jnp.float32) * D ** (-0.25)
    return values.astype(jnp.bfloat16)


def draw_queries(key, part):
    values = jax.random.normal(jax.random.fold_in(key, 12), (QUERIES, LQ, D), jnp.float32) * D ** (-0.25)
    return values.astype(jnp.bfloat16)


def place_ends(result, own_key, low, high):
    index_at = [jax.random.randint(jax.random.fold_in(own_key, axis), (), 0, length) for axis, length in enumerate(result.shape)]
    longest = result.shape.index(max(result.shape))
    next_to = index_at[:longest] + [(index_at[longest] + 1) % result.shape[longest]] + index_at[longest + 1:]
    return result.at[tuple(index_at)].set(low).at[tuple(next_to)].set(high)


def setup_inputs(seed: int = 0) -> dict:
    seeds = jax.random.split(jax.random.key(seed), 4)
    return {
        "queries": draw_queries(jax.random.fold_in(seeds[3], 71), 0),
        "labels": place_ends(jax.random.randint(seeds[1], (QUERIES,), 0, PAGES), jax.random.fold_in(seeds[1], 1), 0, PAGES - 1).astype(jnp.int32),
        "pages": draw_pages(jax.random.fold_in(seeds[3], 71), 0),
    }


def reference(queries, labels, pages):
    flat_rows = queries.reshape(QUERIES * LQ, D)

    def visit(query_grad, inputs):
        page_block, page_number = inputs
        scores = jnp.dot(flat_rows, page_block.T, preferred_element_type=jnp.float32)
        weights = jax.nn.softmax(scores, axis=-1)
        matched = jnp.sum(weights * scores, axis=-1)
        summed = matched.reshape(QUERIES, LQ).sum(axis=1)
        signs = jnp.where(labels == page_number, jnp.float32(1.0), jnp.float32(-1.0))
        logits = summed - jnp.float32(LQ)
        grad_score = -signs * jax.nn.sigmoid(-signs * logits)
        row_grad = jnp.broadcast_to(grad_score[:, None], (QUERIES, LQ)).reshape(QUERIES * LQ)
        dscore = (row_grad[:, None] * weights * (1.0 + scores - matched[:, None])).astype(jnp.bfloat16)
        query_grad = query_grad + jnp.dot(dscore, page_block, preferred_element_type=jnp.float32)
        page_grad = jnp.dot(dscore.T, flat_rows, preferred_element_type=jnp.float32)
        return query_grad, page_grad

    start_grad = jnp.zeros((QUERIES * LQ, D), jnp.float32)
    numbers = jnp.arange(PAGES, dtype=jnp.int32)
    query_grad, page_grads = lax.scan(visit, start_grad, (pages, numbers))
    return query_grad.reshape(QUERIES, LQ, D), page_grads
```

```python
import functools

import jax
import jax.numpy as jnp
from jax import lax
from jax.experimental import pallas as pl
from jax.experimental.pallas import tpu as pltpu
from jax.sharding import PartitionSpec as P

LOG2E = 1.4426950408889634
LN2 = 0.6931471805599453
LQ = 32
RB = 512
TR = 32
HW = 256


def compute_kernel(lab_ref, q_ref, p_ref, first_ref, gp_ref, gq_ref, q2, p2, pt, s0, s1, m0, m1, e0, d0, d1, gacc):
    pages, lp, dd = p_ref.shape
    rows = q_ref.shape[0]
    rb = RB
    nblk = rows // rb
    first = first_ref[0]
    sbuf, mbuf, dbuf = (s0, s1), (m0, m1), (d0, d1)

    def split(i, _):
        at = pl.ds(pl.multiple_of(i * 256, 256), 256)
        x = q_ref[at, :].astype(jnp.float32) * LOG2E
        hi = x.astype(jnp.bfloat16)
        q2[at, :dd] = hi
        q2[at, dd:] = (x - hi.astype(jnp.float32)).astype(jnp.bfloat16)
        return 0
    lax.fori_loop(0, rows // 256, split, 0)
    for p in range(pages):
        for c in range(0, lp, 256):
            blk = p_ref[p, c:c + 256, :]
            p2[p, c:c + 256, :dd] = blk
            p2[p, c:c + 256, dd:] = blk
            pt[p, :, c:c + 256] = blk.T
    gp_ref[...] = jnp.zeros_like(gp_ref)
    gacc[...] = jnp.zeros_like(gacc)
    d1[...] = jnp.zeros_like(d1)

    def units_a(r, p, s_ref, m_ref):
        at = pl.ds(pl.multiple_of(r * rb, rb), rb)
        out = []
        state = {}

        def chunk(c):
            s = lax.dot_general(p2[p, c:c + 256, :], q2[at, :], (((1,), (1,)), ((), ())), preferred_element_type=jnp.float32)
            s_ref[c:c + 256, :] = s
            m = jnp.max(s.reshape(32, 8, rb), axis=0)
            state["m"] = m if c == 0 else jnp.maximum(state["m"], m)
            if c + 256 == lp:
                m_ref[...] = state["m"]
        return [functools.partial(chunk, c) for c in range(0, lp, 256)]

    def units_bc(r, p, s_ref, m_ref, d_ref):
        lane = lax.broadcasted_iota(jnp.int32, (8, 128), 1)
        st = {}
        b, c_ = [], []

        def start(h):
            m = m_ref[:, h:h + HW]
            m = jnp.broadcast_to(jnp.max(m, axis=0, keepdims=True), m.shape)
            st["m", h] = m
            st["l", h] = jnp.zeros((8, HW), jnp.float32)
            st["n", h] = jnp.zeros((8, HW), jnp.float32)

        def bt(h, k):
            if k == 0:
                start(h)
            y = s_ref[k:k + TR, h:h + HW].reshape(TR // 8, 8, HW)
            x = y - st["m", h][None]
            e = jnp.exp2(x)
            e0[k:k + TR, h:h + HW] = e.reshape(TR, HW)
            st["l", h] += jnp.sum(e, axis=0)
            st["n", h] += jnp.sum(e * x, axis=0)
            if k + TR == lp:
                finish(h)

        def finish(h):
            l = jnp.broadcast_to(jnp.sum(st["l", h], axis=0, keepdims=True), (8, HW))
            n = jnp.broadcast_to(jnp.sum(st["n", h], axis=0, keepdims=True), (8, HW))
            inv = 1.0 / l
            m2 = st["m", h] + n * inv
            tot = []
            for g in range(0, HW, 128):
                t = m2[:, g:g + 128]
                for w in (1, 2, 4, 8, 16):
                    up = pltpu.roll(t, 128 - w, 1)
                    dn = pltpu.roll(t, w, 1)
                    t = t + jnp.where((lane & w) == 0, up, dn)
                tot.append(t)
            score = jnp.concatenate(tot, axis=1) * LN2
            at = pl.ds(pl.multiple_of(r * rb + h, HW), HW)
            lab = lab_ref[:, at]
            sign = jnp.where(lab == first + p, 1.0, -1.0).astype(jnp.float32)
            g = -sign / (1.0 + jnp.exp(sign * (score - float(LQ))))
            st["a", h] = g * inv * LN2
            st["c", h] = m2 - LOG2E

        def ct(h, k):
            y = s_ref[k:k + TR, h:h + HW].reshape(TR // 8, 8, HW)
            e = e0[k:k + TR, h:h + HW].reshape(TR // 8, 8, HW)
            d = (e * st["a", h][None]) * (y - st["c", h][None])
            d_ref[k:k + TR, h:h + HW] = d.reshape(TR, HW).astype(jnp.bfloat16)

        us = []
        for h in range(0, rb, HW):
            us += [functools.partial(bt, h, k) for k in range(0, lp, TR)]
        for h in range(0, rb, HW):
            us += [functools.partial(ct, h, k) for k in range(0, lp, TR)]
        return us

    def units_d(r, p, d_ref):
        at = pl.ds(pl.multiple_of(r * rb, rb), rb)
        st = {}

        def gq(c):
            t = jnp.dot(pt[p, :, c:c + 256], d_ref[c:c + 256, :], preferred_element_type=jnp.float32)
            st["g"] = t if c == 0 else st["g"] + t
            if c + 256 == lp:
                if p == 0:
                    gacc[...] = st["g"]
                elif p < pages - 1:
                    gacc[...] += st["g"]
                else:
                    tot = gacc[...] + st["g"]
                    for k in range(0, rb, 128):
                        gq_ref[pl.ds(pl.multiple_of(r * rb + k, 128), 128), :] = tot[:, k:k + 128].T.astype(gq_ref.dtype)

        def gp(c):
            gp_ref[p, c:c + 256, :] += jnp.dot(d_ref[c:c + 256, :], q_ref[at, :], preferred_element_type=jnp.float32)

        us = []
        for c in range(0, lp, 256):
            us += [functools.partial(gq, c), functools.partial(gp, c)]
        return us

    def weave(vec, mxu):
        n, k = len(vec), len(mxu)
        j = 0
        for i, u in enumerate(vec):
            while j < k and j * n <= i * k:
                mxu[j]()
                j += 1
            u()
        while j < k:
            mxu[j]()
            j += 1

    for u in units_a(0, 0, s0, m0):
        u()

    def body(r, _):
        for p in range(pages):
            nr = r if p + 1 < pages else jnp.minimum(r + 1, nblk - 1)
            a = units_a(nr, (p + 1) % pages, sbuf[(p + 1) % 2], mbuf[(p + 1) % 2])
            bc = units_bc(r, p, sbuf[p % 2], mbuf[p % 2], dbuf[p % 2])
            d = units_d(r if p > 0 else jnp.maximum(r - 1, 0), (p - 1) % pages, dbuf[(p - 1) % 2])
            mx = []
            for i in range(4):
                mx += [d[2 * i], d[2 * i + 1], a[i]]
            weave(bc, mx)
        return 0

    lax.fori_loop(0, nblk, body, 0)
    for u in units_d(nblk - 1, pages - 1, dbuf[(pages - 1) % 2]):
        u()


def compute(lab, q, p, first):
    pages, lp, dd = p.shape
    rows = q.shape[0]
    vm = pl.BlockSpec(memory_space=pltpu.VMEM)
    return pl.pallas_call(
        compute_kernel,
        out_shape=(jax.ShapeDtypeStruct((pages, lp, dd), jnp.float32), jax.ShapeDtypeStruct((rows, dd), jnp.bfloat16)),
        in_specs=[vm, vm, vm, pl.BlockSpec(memory_space=pltpu.SMEM)],
        out_specs=(vm, vm),
        scratch_shapes=[
            pltpu.VMEM((rows, 2 * dd), jnp.bfloat16),
            pltpu.VMEM((pages, lp, 2 * dd), jnp.bfloat16),
            pltpu.VMEM((pages, dd, lp), jnp.bfloat16),
            pltpu.VMEM((lp, RB), jnp.float32), pltpu.VMEM((lp, RB), jnp.float32),
            pltpu.VMEM((8, RB), jnp.float32), pltpu.VMEM((8, RB), jnp.float32),
            pltpu.VMEM((lp, RB), jnp.float32),
            pltpu.VMEM((lp, RB), jnp.bfloat16), pltpu.VMEM((lp, RB), jnp.bfloat16),
            pltpu.VMEM((dd, RB), jnp.float32),
        ],
        compiler_params=pltpu.CompilerParams(vmem_limit_bytes=60 << 20),
        name="late_interaction",
    )(lab, q, p, first)


def in_order(pieces, dim):
    pieces = jnp.moveaxis(pieces, 0, dim)
    shape = pieces.shape
    return pieces.reshape(*shape[:dim], shape[dim] * shape[dim + 1], *shape[dim + 2 :])


def sent_to_all(shard, axis):
    peers = lax.axis_size(axis)
    return lax.all_to_all(
        jnp.broadcast_to(shard[None], (peers, *shard.shape)), axis, 0, 0, tiled=True
    )


def gather_directly(shard, axis, dim):
    return in_order(sent_to_all(shard, axis), dim)


def in_blocks(shard, dim, peers):
    before, after = (shard.shape[:dim], shard.shape[dim + 1 :])
    return jnp.moveaxis(shard.reshape(*before, peers, -1, *after), dim, 0)


def summed(shard, axis, dim):
    peers = lax.axis_size(axis)
    pieces = lax.all_to_all(in_blocks(shard, dim, peers), axis, 0, 0, tiled=True)
    return jnp.sum(pieces.astype(jnp.float32), axis=0)


def shards(queries, labels, pages):
    first = lax.axis_index(("dp", "inner")) * pages.shape[0]
    token_count, width = queries.shape[1:]
    rows = gather_directly(gather_directly(queries, "inner", 0), "dp", 0)
    labs = gather_directly(gather_directly(labels, "inner", 0), "dp", 0)
    count = rows.shape[0]
    flat = rows.reshape(count * token_count, width)
    lab8 = jnp.broadcast_to(jnp.repeat(labs, token_count)[None], (8, count * token_count))
    grad_pages, partial = compute(lab8, flat, pages, first.astype(jnp.int32).reshape(1))
    partial = partial.reshape(count, token_count, width)
    grad_queries = summed(summed(partial, "dp", 0), "inner", 0)
    return grad_queries, grad_pages


def solution(mesh):
    placed = (P(("dp", "inner"), None, None), P(("dp", "inner")), P(("dp", "inner"), None, None))
    return jax.shard_map(
        shards,
        mesh=mesh,
        in_specs=placed,
        out_specs=(P(("dp", "inner"), None, None), P(("dp", "inner"), None, None)),
        check_vma=False,
    )
```

```python
import functools

import jax
import jax.numpy as jnp
from jax import lax
from jax.experimental import pallas as pl
from jax.experimental.pallas import tpu as pltpu
from jax.sharding import PartitionSpec as P

LOG2E = 1.4426950408889634
LN2 = 0.6931471805599453
LQ = 32
RB = 512
TR = 1024
HW = 256


MESH = pl.DeviceIdType.MESH


def step_kernel(lab_ref, q_ref, p_hbm, gp_ref, out_ref, p_ref, q_buf, l_buf, part, recv, q2, p2, pt, s0, s1, m0, m1, e0, d0, d1, gacc,
                p_sem, q_sem, l_sem, r_sem, qs_sem, ls_sem, rs_sem):
    pages, lp, dd = p_ref.shape
    ndp, nin = lax.axis_size("dp"), lax.axis_size("inner")
    dp, inner = lax.axis_index("dp"), lax.axis_index("inner")
    me = dp * nin + inner
    total = ndp * nin
    rb = RB
    nblk = ndp
    first = me * pages
    sbuf, mbuf, dbuf = (s0, s1), (m0, m1), (d0, d1)

    barrier = pltpu.get_barrier_semaphore()
    fetch = pltpu.make_async_copy(p_hbm, p_ref, p_sem)
    fetch.start()

    def greet(k, _):
        t = lax.rem(me + k, total)
        pl.semaphore_signal(barrier, inc=1, device_id={"dp": t // nin, "inner": lax.rem(t, nin)}, device_id_type=MESH)
        return 0
    lax.fori_loop(1, total, greet, 0)

    own = pl.ds(pl.multiple_of(me * LQ, LQ), LQ)
    q_buf[own, :] = q_ref[0]
    l_buf[pl.ds(me, 1), :, :] = jnp.full((1, 1, 128), lab_ref[0], jnp.int32)
    gp_ref[...] = jnp.zeros_like(gp_ref)
    gacc[...] = jnp.zeros_like(gacc)
    d1[...] = jnp.zeros_like(d1)
    fetch.wait()
    for p in range(pages):
        for c in range(0, lp, 256):
            blk = p_ref[p, c:c + 256, :]
            p2[p, c:c + 256, :dd] = blk
            p2[p, c:c + 256, dd:] = blk
            pt[p, :, c:c + 256] = blk.T
    pl.semaphore_wait(barrier, total - 1)

    def q_copy(t_dp, t_in):
        return pltpu.make_async_remote_copy(
            src_ref=q_buf.at[own, :], dst_ref=q_buf.at[own, :], send_sem=qs_sem, recv_sem=q_sem.at[dp],
            device_id={"dp": t_dp, "inner": t_in}, device_id_type=MESH)

    def l_copy(t_dp, t_in):
        return pltpu.make_async_remote_copy(
            src_ref=l_buf.at[me], dst_ref=l_buf.at[me], send_sem=ls_sem, recv_sem=l_sem.at[dp],
            device_id={"dp": t_dp, "inner": t_in}, device_id_type=MESH)

    def part_copy(r, t_in):
        rows = pl.ds(pl.multiple_of(r * rb + t_in * LQ, LQ), LQ)
        return pltpu.make_async_remote_copy(
            src_ref=part.at[rows, :], dst_ref=recv.at[me], send_sem=rs_sem, recv_sem=r_sem,
            device_id={"dp": r, "inner": t_in}, device_id_type=MESH)

    def share(k, _):
        t_dp, t_in = lax.rem(dp + ndp - k // nin, ndp), lax.rem(inner + k, nin)
        q_copy(t_dp, t_in).start()
        l_copy(t_dp, t_in).start()
        return 0
    lax.fori_loop(1, 2 * nin, share, 0)

    def block(k):
        return lax.rem(dp + k, ndp)

    def arrived(k, r, count):
        qs, ls = q_buf.at[pl.ds(0, count * LQ), :], l_buf.at[pl.ds(0, count)]
        pltpu.make_async_copy(qs, qs, q_sem.at[r]).wait()
        pltpu.make_async_copy(ls, ls, l_sem.at[r]).wait()

    def split(r):
        for c in range(0, rb, 256):
            at = pl.ds(pl.multiple_of(r * rb + c, 256), 256)
            x = q_buf[at, :].astype(jnp.float32) * LOG2E
            hi = x.astype(jnp.bfloat16)
            q2[at, :dd] = hi
            q2[at, dd:] = (x - hi.astype(jnp.float32)).astype(jnp.bfloat16)

    def send(k):
        r = block(k)

        def one(i, _):
            t_in = lax.rem(inner + i, nin)

            @pl.when(i + k > 0)
            def _():
                part_copy(r, t_in).start()
            return 0
        lax.fori_loop(0, nin, one, 0)

    def units_a(r, p, s_ref, m_ref):
        at = pl.ds(pl.multiple_of(r * rb, rb), rb)

        def scores():
            s = lax.dot_general(p2[p], q2[at, :], (((1,), (1,)), ((), ())), preferred_element_type=jnp.float32)
            s_ref[...] = s
            m_ref[...] = jnp.max(s.reshape(lp // 8, 8, rb), axis=0)
        return [scores]

    def units_bc(r, p, s_ref, m_ref, d_ref):
        lane = lax.broadcasted_iota(jnp.int32, (8, 128), 1)
        st = {}
        b, c_ = [], []

        def start(h):
            m = m_ref[:, h:h + HW]
            m = jnp.broadcast_to(jnp.max(m, axis=0, keepdims=True), m.shape)
            st["m", h] = m
            st["l", h] = jnp.zeros((8, HW), jnp.float32)
            st["n", h] = jnp.zeros((8, HW), jnp.float32)

        def bt(h, k):
            if k == 0:
                start(h)
            y = s_ref[k:k + TR, h:h + HW].reshape(TR // 8, 8, HW)
            x = y - st["m", h][None]
            e = jnp.exp2(x)
            e0[k:k + TR, h:h + HW] = e.reshape(TR, HW)
            st["l", h] += jnp.sum(e, axis=0)
            st["n", h] += jnp.sum(e * x, axis=0)
            if k + TR == lp:
                finish(h)

        def finish(h):
            l = jnp.broadcast_to(jnp.sum(st["l", h], axis=0, keepdims=True), (8, HW))
            n = jnp.broadcast_to(jnp.sum(st["n", h], axis=0, keepdims=True), (8, HW))
            inv = 1.0 / l
            m2 = st["m", h] + n * inv
            tot = []
            for g in range(0, HW, 128):
                t = m2[:, g:g + 128]
                for w in (1, 2, 4, 8, 16):
                    up = pltpu.roll(t, 128 - w, 1)
                    dn = pltpu.roll(t, w, 1)
                    t = t + jnp.where((lane & w) == 0, up, dn)
                tot.append(t)
            score = jnp.concatenate(tot, axis=1) * LN2
            lab = []
            for g in range(0, HW, 128):
                rows = [jnp.broadcast_to(l_buf[r * (rb // LQ) + (h + g) // LQ + j], (8, 128)) for j in range(128 // LQ)]
                row = rows[-1]
                for j in range(128 // LQ - 2, -1, -1):
                    row = jnp.where(lane < (j + 1) * LQ, rows[j], row)
                lab.append(row)
            lab = jnp.concatenate(lab, axis=1)
            sign = jnp.where(lab == first + p, 1.0, -1.0).astype(jnp.float32)
            g = -sign / (1.0 + jnp.exp(sign * (score - float(LQ))))
            st["a", h] = g * inv * LN2
            st["c", h] = m2 - LOG2E

        def ct(h, k):
            y = s_ref[k:k + TR, h:h + HW].reshape(TR // 8, 8, HW)
            e = e0[k:k + TR, h:h + HW].reshape(TR // 8, 8, HW)
            d = (e * st["a", h][None]) * (y - st["c", h][None])
            d_ref[k:k + TR, h:h + HW] = d.reshape(TR, HW).astype(jnp.bfloat16)

        us = []
        for h in range(0, rb, HW):
            us += [functools.partial(bt, h, k) for k in range(0, lp, TR)]
        for h in range(0, rb, HW):
            us += [functools.partial(ct, h, k) for k in range(0, lp, TR)]
        return us

    def units_d(r, p, d_ref):
        at = pl.ds(pl.multiple_of(r * rb, rb), rb)

        def gq():
            t = jnp.dot(pt[p], d_ref[...], preferred_element_type=jnp.float32)
            if p == 0:
                gacc[...] = t
            elif p < pages - 1:
                gacc[...] += t
            else:
                part[at, :] = (gacc[...] + t).T.astype(part.dtype)

        def gp():
            gp_ref[p] += jnp.dot(d_ref[...], q_buf[at, :], preferred_element_type=jnp.float32)

        return [gq, gp]

    def weave(vec, mxu):
        n, k = len(vec), len(mxu)
        j = 0
        for i, u in enumerate(vec):
            while j < k and j * n <= i * k:
                mxu[j]()
                j += 1
            u()
        while j < k:
            mxu[j]()
            j += 1

    arrived(0, dp, nin - 1)
    split(dp)
    for u in units_a(dp, 0, s0, m0):
        u()

    def body(k, _):
        r = block(k)
        nxt = block(jnp.minimum(k + 1, nblk - 1))
        prev = block(jnp.maximum(k - 1, 0))

        @pl.when(k + 1 < nblk)
        def _():
            arrived(k + 1, nxt, nin)

        @pl.when(k + 2 < nblk)
        def _():
            lax.fori_loop((k + 2) * nin, (k + 3) * nin, share, 0)
        split(nxt)
        for p in range(pages):
            nr = r if p + 1 < pages else nxt
            a = units_a(nr, (p + 1) % pages, sbuf[(p + 1) % 2], mbuf[(p + 1) % 2])
            bc = units_bc(r, p, sbuf[p % 2], mbuf[p % 2], dbuf[p % 2])
            d = units_d(r if p > 0 else prev, (p - 1) % pages, dbuf[(p - 1) % 2])
            weave(bc, d + a)

        @pl.when(k > 0)
        def _():
            send(k - 1)
        return 0

    lax.fori_loop(0, nblk, body, 0)
    last = block(nblk - 1)
    for u in units_d(last, pages - 1, dbuf[(pages - 1) % 2]):
        u()
    recv[pl.ds(me, 1), :, :] = part[own, :][None]
    send(nblk - 1)

    others = recv.at[pl.ds(0, total - 1)]
    pltpu.make_async_copy(others, others, r_sem).wait()

    def add(i, acc):
        blk = recv[pl.ds(pl.multiple_of(i * 8, 8), 8), :, :].astype(jnp.float32)
        return acc + jnp.sum(blk, axis=0)
    out_ref[0] = lax.fori_loop(0, total // 8, add, jnp.zeros((LQ, dd), jnp.float32))

    pltpu.make_async_copy(others, others, rs_sem).wait()
    pltpu.make_async_copy(others, others, qs_sem).wait()
    labels = l_buf.at[pl.ds(0, total - 1)]
    pltpu.make_async_copy(labels, labels, ls_sem).wait()


def shards(queries, labels, pages):
    count, lp, dd = pages.shape
    total = lax.axis_size("dp") * lax.axis_size("inner")
    rows = total * LQ
    vm = pl.BlockSpec(memory_space=pltpu.VMEM)
    f32, bf16 = jnp.float32, jnp.bfloat16
    grad_pages, grad_queries = pl.pallas_call(
        step_kernel,
        out_shape=(jax.ShapeDtypeStruct(pages.shape, f32), jax.ShapeDtypeStruct(queries.shape, f32)),
        in_specs=[pl.BlockSpec(memory_space=pltpu.SMEM), vm, pl.BlockSpec(memory_space=pl.ANY)],
        out_specs=(vm, vm),
        scratch_shapes=[
            pltpu.VMEM((count, lp, dd), bf16),
            pltpu.VMEM((rows, dd), bf16),
            pltpu.VMEM((total, 1, 128), jnp.int32),
            pltpu.VMEM((rows, dd), bf16),
            pltpu.VMEM((total, LQ, dd), bf16),
            pltpu.VMEM((rows, 2 * dd), bf16),
            pltpu.VMEM((count, lp, 2 * dd), bf16),
            pltpu.VMEM((count, dd, lp), bf16),
            pltpu.VMEM((lp, RB), f32), pltpu.VMEM((lp, RB), f32),
            pltpu.VMEM((8, RB), f32), pltpu.VMEM((8, RB), f32),
            pltpu.VMEM((lp, RB), f32),
            pltpu.VMEM((lp, RB), bf16), pltpu.VMEM((lp, RB), bf16),
            pltpu.VMEM((dd, RB), f32),
            pltpu.SemaphoreType.DMA,
            pltpu.SemaphoreType.DMA((8,)),
            pltpu.SemaphoreType.DMA((8,)),
            pltpu.SemaphoreType.DMA,
            pltpu.SemaphoreType.DMA,
            pltpu.SemaphoreType.DMA,
            pltpu.SemaphoreType.DMA,
        ],
        compiler_params=pltpu.CompilerParams(vmem_limit_bytes=36 << 20, collective_id=0, has_side_effects=True),
        name="late_interaction",
    )(labels, queries, pages)
    return grad_queries, grad_pages


def solution(mesh):
    placed = (P(("dp", "inner"), None, None), P(("dp", "inner")), P(("dp", "inner"), None, None))
    return jax.shard_map(
        shards,
        mesh=mesh,
        in_specs=placed,
        out_specs=(P(("dp", "inner"), None, None), P(("dp", "inner"), None, None)),
        check_vma=False,
    )
```

```python
import functools

import jax
import jax.numpy as jnp
from jax import lax
from jax.experimental import pallas as pl
from jax.experimental.pallas import tpu as pltpu
from jax.sharding import PartitionSpec as P

LOG2E = 1.4426950408889634
LN2 = 0.6931471805599453
LQ = 32
RB = 512
TR = 256
HW = 512


MESH = pl.DeviceIdType.MESH


def step_kernel(lab_ref, q_ref, p_hbm, gp_ref, out_ref, p_ref, q_buf, l_buf, part, recv, q2, p2, pt, s0, s1, m0, m1, e0, d0, d1, gacc,
                p_sem, q_sem, l_sem, r_sem, qs_sem, ls_sem, rs_sem):
    pages, lp, dd = p_ref.shape
    ndp, nin = lax.axis_size("dp"), lax.axis_size("inner")
    dp, inner = lax.axis_index("dp"), lax.axis_index("inner")
    me = dp * nin + inner
    total = ndp * nin
    rb = RB
    nblk = ndp
    first = me * pages
    sbuf, mbuf, dbuf = (s0, s1), (m0, m1), (d0, d1)

    barrier = pltpu.get_barrier_semaphore()
    fetch = pltpu.make_async_copy(p_hbm, p_ref, p_sem)
    fetch.start()

    own = pl.ds(pl.multiple_of(me * LQ, LQ), LQ)
    q_buf[own, :] = q_ref[0]
    l_buf[pl.ds(me, 1), :, :] = jnp.full((1, 1, 128), lab_ref[0], jnp.int32)

    def greet(t_dp, t_in):
        pl.semaphore_signal(barrier, inc=1, device_id={"dp": t_dp, "inner": t_in}, device_id_type=MESH)

    dps = [lax.rem(dp + a, ndp) for a in range(8)]

    def greet_all(b, _):
        t_in = lax.rem(inner + b, nin)
        for t_dp in dps:
            greet(t_dp, t_in)
        return 0
    lax.fori_loop(1, nin, greet_all, 0)
    for t_dp in dps[1:]:
        greet(t_dp, inner)
    pl.semaphore_wait(barrier, total - 1)

    def q_copy(t_dp, t_in):
        return pltpu.make_async_remote_copy(
            src_ref=q_buf.at[own, :], dst_ref=q_buf.at[own, :], send_sem=qs_sem, recv_sem=q_sem.at[dp],
            device_id={"dp": t_dp, "inner": t_in}, device_id_type=MESH)

    def l_copy(t_dp, t_in):
        return pltpu.make_async_remote_copy(
            src_ref=l_buf.at[me], dst_ref=l_buf.at[me], send_sem=ls_sem, recv_sem=l_sem.at[dp],
            device_id={"dp": t_dp, "inner": t_in}, device_id_type=MESH)

    def part_copy(r, t_in):
        rows = pl.ds(pl.multiple_of(r * rb + t_in * LQ, LQ), LQ)
        return pltpu.make_async_remote_copy(
            src_ref=part.at[rows, :], dst_ref=recv.at[me], send_sem=rs_sem, recv_sem=r_sem.at[dp],
            device_id={"dp": r, "inner": t_in}, device_id_type=MESH)

    def share(k, start):
        t_dp = lax.rem(dp + ndp - k, ndp)

        def one(i, _):
            t_in = lax.rem(inner + i, nin)
            q_copy(t_dp, t_in).start()
            l_copy(t_dp, t_in).start()
            return 0
        lax.fori_loop(start, nin, one, 0)
    share(0, 1)
    share(1, 0)

    gp_ref[...] = jnp.zeros_like(gp_ref)
    gacc[...] = jnp.zeros_like(gacc)
    d1[...] = jnp.zeros_like(d1)
    fetch.wait()
    for p in range(pages):
        p2[p, :, :dd] = p_ref[p]
        p2[p, :, dd:] = p_ref[p]
        pt[p] = p_ref[p].T
    share(2, 0)
    share(3, 0)

    def block(k):
        return lax.rem(dp + k, ndp)

    def arrived(k, r, count):
        qs, ls = q_buf.at[pl.ds(0, count * LQ), :], l_buf.at[pl.ds(0, count)]
        pltpu.make_async_copy(qs, qs, q_sem.at[r]).wait()
        pltpu.make_async_copy(ls, ls, l_sem.at[r]).wait()

    def split(r):
        for c in range(0, rb, 256):
            at = pl.ds(pl.multiple_of(r * rb + c, 256), 256)
            x = q_buf[at, :].astype(jnp.float32) * LOG2E
            hi = x.astype(jnp.bfloat16)
            q2[at, :dd] = hi
            q2[at, dd:] = (x - hi.astype(jnp.float32)).astype(jnp.bfloat16)

    def send(k):
        r = block(k)

        def one(i, _):
            t_in = lax.rem(inner + i, nin)

            @pl.when(i + k > 0)
            def _():
                part_copy(r, t_in).start()
            return 0
        lax.fori_loop(0, nin, one, 0)

    def units_a(r, p, s_ref, m_ref):
        at = pl.ds(pl.multiple_of(r * rb, rb), rb)

        def scores():
            s = lax.dot_general(p2[p], q2[at, :], (((1,), (1,)), ((), ())), preferred_element_type=jnp.float32)
            s_ref[...] = s
            m_ref[...] = jnp.max(s.reshape(lp // 8, 8, rb), axis=0)
        return [scores]

    def units_bc(r, p, s_ref, m_ref, d_ref):
        lane = lax.broadcasted_iota(jnp.int32, (8, 128), 1)
        st = {}
        b, c_ = [], []

        def start(h):
            m = m_ref[:, h:h + HW]
            m = jnp.broadcast_to(jnp.max(m, axis=0, keepdims=True), m.shape)
            st["m", h] = m
            st["l", h] = jnp.zeros((8, HW), jnp.float32)
            st["n", h] = jnp.zeros((8, HW), jnp.float32)

        def bt(h, k):
            if k == 0:
                start(h)
            y = s_ref[k:k + TR, h:h + HW].reshape(TR // 8, 8, HW)
            x = y - st["m", h][None]
            e = jnp.exp2(x)
            e0[k:k + TR, h:h + HW] = e.reshape(TR, HW)
            st["l", h] += jnp.sum(e, axis=0)
            st["n", h] += jnp.sum(e * x, axis=0)
            if k + TR == lp:
                finish(h)

        def finish(h):
            l = jnp.broadcast_to(jnp.sum(st["l", h], axis=0, keepdims=True), (8, HW))
            n = jnp.broadcast_to(jnp.sum(st["n", h], axis=0, keepdims=True), (8, HW))
            inv = 1.0 / l
            m2 = st["m", h] + n * inv
            tot = []
            for g in range(0, HW, 128):
                t = m2[:, g:g + 128]
                for w in (1, 2, 4, 8, 16):
                    up = pltpu.roll(t, 128 - w, 1)
                    dn = pltpu.roll(t, w, 1)
                    t = t + jnp.where((lane & w) == 0, up, dn)
                tot.append(t)
            score = jnp.concatenate(tot, axis=1) * LN2
            lab = []
            for g in range(0, HW, 128):
                rows = [jnp.broadcast_to(l_buf[r * (rb // LQ) + (h + g) // LQ + j], (8, 128)) for j in range(128 // LQ)]
                row = rows[-1]
                for j in range(128 // LQ - 2, -1, -1):
                    row = jnp.where(lane < (j + 1) * LQ, rows[j], row)
                lab.append(row)
            lab = jnp.concatenate(lab, axis=1)
            sign = jnp.where(lab == first + p, 1.0, -1.0).astype(jnp.float32)
            g = -sign / (1.0 + jnp.exp(sign * (score - float(LQ))))
            st["a", h] = g * inv * LN2
            st["c", h] = m2 - LOG2E

        def ct(h, k):
            y = s_ref[k:k + TR, h:h + HW].reshape(TR // 8, 8, HW)
            e = e0[k:k + TR, h:h + HW].reshape(TR // 8, 8, HW)
            d = (e * st["a", h][None]) * (y - st["c", h][None])
            d_ref[k:k + TR, h:h + HW] = d.reshape(TR, HW).astype(jnp.bfloat16)

        us = []
        for h in range(0, rb, HW):
            us += [functools.partial(bt, h, k) for k in range(0, lp, TR)]
        for h in range(0, rb, HW):
            us += [functools.partial(ct, h, k) for k in range(0, lp, TR)]
        return us

    def units_d(r, p, d_ref):
        at = pl.ds(pl.multiple_of(r * rb, rb), rb)

        def gq():
            t = jnp.dot(pt[p], d_ref[...], preferred_element_type=jnp.float32)
            if p == 0:
                gacc[...] = t
            elif p < pages - 1:
                gacc[...] += t
            else:
                part[at, :] = (gacc[...] + t).T.astype(part.dtype)

        def gp():
            gp_ref[p] += jnp.dot(d_ref[...], q_buf[at, :], preferred_element_type=jnp.float32)

        return [gq, gp]

    def weave(vec, mxu):
        n, k = len(vec), len(mxu)
        j = 0
        for i, u in enumerate(vec):
            while j < k and j * n <= i * k:
                mxu[j]()
                j += 1
            u()
        while j < k:
            mxu[j]()
            j += 1

    arrived(0, dp, nin - 1)
    split(dp)
    for u in units_a(dp, 0, s0, m0):
        u()

    def body(k, _):
        r = block(k)
        nxt = block(jnp.minimum(k + 1, nblk - 1))
        prev = block(jnp.maximum(k - 1, 0))

        @pl.when(k + 1 < nblk)
        def _():
            arrived(k + 1, nxt, nin)

        @pl.when(k + 4 < nblk)
        def _():
            share(k + 4, 0)
        split(nxt)
        for p in range(pages):
            nr = r if p + 1 < pages else nxt
            a = units_a(nr, (p + 1) % pages, sbuf[(p + 1) % 2], mbuf[(p + 1) % 2])
            bc = units_bc(r, p, sbuf[p % 2], mbuf[p % 2], dbuf[p % 2])
            d = units_d(r if p > 0 else prev, (p - 1) % pages, dbuf[(p - 1) % 2])
            weave(bc, d + a)

        @pl.when(k > 0)
        def _():
            send(k - 1)
        return 0

    lax.fori_loop(0, nblk, body, 0)
    last = block(nblk - 1)
    grad_q, grad_p = units_d(last, pages - 1, dbuf[(pages - 1) % 2])
    grad_q()
    recv[pl.ds(me, 1), :, :] = part[own, :][None]
    send(nblk - 1)
    grad_p()

    def landed(g, count):
        got = recv.at[pl.ds(0, count)]
        pltpu.make_async_copy(got, got, r_sem.at[g]).wait()

    def summed(g):
        terms = recv[pl.ds(pl.multiple_of(g * 16, 16), 16), :, :]
        return jnp.sum(terms.astype(jnp.float32), axis=0)

    landed(dp, nin - 1)
    for a in range(2, 8):
        landed(dps[a], nin)
    tot = summed(dp)
    for a in range(2, 8):
        tot += summed(dps[a])
    landed(dps[1], nin)
    out_ref[0] = tot + summed(dps[1])

    others = recv.at[pl.ds(0, total - 1)]
    pltpu.make_async_copy(others, others, rs_sem).wait()
    pltpu.make_async_copy(others, others, qs_sem).wait()
    labels = l_buf.at[pl.ds(0, total - 1)]
    pltpu.make_async_copy(labels, labels, ls_sem).wait()


def shards(queries, labels, pages):
    count, lp, dd = pages.shape
    total = lax.axis_size("dp") * lax.axis_size("inner")
    rows = total * LQ
    vm = pl.BlockSpec(memory_space=pltpu.VMEM)
    f32, bf16 = jnp.float32, jnp.bfloat16
    grad_pages, grad_queries = pl.pallas_call(
        step_kernel,
        out_shape=(jax.ShapeDtypeStruct(pages.shape, f32), jax.ShapeDtypeStruct(queries.shape, f32)),
        in_specs=[pl.BlockSpec(memory_space=pltpu.SMEM), vm, pl.BlockSpec(memory_space=pl.ANY)],
        out_specs=(vm, vm),
        scratch_shapes=[
            pltpu.VMEM((count, lp, dd), bf16),
            pltpu.VMEM((rows, dd), bf16),
            pltpu.VMEM((total, 1, 128), jnp.int32),
            pltpu.VMEM((rows, dd), bf16),
            pltpu.VMEM((total, LQ, dd), bf16),
            pltpu.VMEM((rows, 2 * dd), bf16),
            pltpu.VMEM((count, lp, 2 * dd), bf16),
            pltpu.VMEM((count, dd, lp), bf16),
            pltpu.VMEM((lp, RB), f32), pltpu.VMEM((lp, RB), f32),
            pltpu.VMEM((8, RB), f32), pltpu.VMEM((8, RB), f32),
            pltpu.VMEM((lp, RB), f32),
            pltpu.VMEM((lp, RB), bf16), pltpu.VMEM((lp, RB), bf16),
            pltpu.VMEM((dd, RB), f32),
            pltpu.SemaphoreType.DMA,
            pltpu.SemaphoreType.DMA((8,)),
            pltpu.SemaphoreType.DMA((8,)),
            pltpu.SemaphoreType.DMA((8,)),
            pltpu.SemaphoreType.DMA,
            pltpu.SemaphoreType.DMA,
            pltpu.SemaphoreType.DMA,
        ],
        compiler_params=pltpu.CompilerParams(vmem_limit_bytes=36 << 20, collective_id=0, has_side_effects=True),
        name="late_interaction",
    )(labels, queries, pages)
    return grad_queries, grad_pages


def solution(mesh):
    placed = (P(("dp", "inner"), None, None), P(("dp", "inner")), P(("dp", "inner"), None, None))
    return jax.shard_map(
        shards,
        mesh=mesh,
        in_specs=placed,
        out_specs=(P(("dp", "inner"), None, None), P(("dp", "inner"), None, None)),
        check_vma=False,
    )
```

```python
import functools

import jax
import jax.numpy as jnp
from jax import lax
from jax.experimental import pallas as pl
from jax.experimental.pallas import tpu as pltpu
from jax.sharding import PartitionSpec as P

LOG2E = 1.4426950408889634
LN2 = 0.6931471805599453
LQ = 32
RB = 512
TR = 128
HW = 512


MESH = pl.DeviceIdType.MESH


def step_kernel(lab_ref, q_ref, p_hbm, gp_ref, out_ref, p_ref, q_buf, l_buf, part, recv, q2, p2, pt, s0, s1, m0, m1, e0, d0, d1, gacc,
                p_sem, q_sem, l_sem, r_sem, qs_sem, ls_sem, rs_sem):
    pages, lp, dd = p_ref.shape
    ndp, nin = lax.axis_size("dp"), lax.axis_size("inner")
    dp, inner = lax.axis_index("dp"), lax.axis_index("inner")
    me = dp * nin + inner
    total = ndp * nin
    rb = RB
    nblk = ndp
    first = me * pages
    sbuf, mbuf, dbuf = (s0, s1), (m0, m1), (d0, d1)

    barrier = pltpu.get_barrier_semaphore()
    fetch = pltpu.make_async_copy(p_hbm, p_ref, p_sem)
    fetch.start()

    own = pl.ds(pl.multiple_of(me * LQ, LQ), LQ)
    q_buf[own, :] = q_ref[0]
    l_buf[pl.ds(me, 1), :, :] = jnp.full((1, 1, 128), lab_ref[0], jnp.int32)

    def greet(t_dp, t_in):
        pl.semaphore_signal(barrier, inc=1, device_id={"dp": t_dp, "inner": t_in}, device_id_type=MESH)

    dps = [lax.rem(dp + a, ndp) for a in range(8)]

    def greet_all(b, _):
        t_in = lax.rem(inner + b, nin)
        for t_dp in dps:
            greet(t_dp, t_in)
        return 0
    lax.fori_loop(1, nin, greet_all, 0)
    for t_dp in dps[1:]:
        greet(t_dp, inner)
    pl.semaphore_wait(barrier, total - 1)

    def q_copy(t_dp, t_in):
        return pltpu.make_async_remote_copy(
            src_ref=q_buf.at[own, :], dst_ref=q_buf.at[own, :], send_sem=qs_sem, recv_sem=q_sem.at[dp],
            device_id={"dp": t_dp, "inner": t_in}, device_id_type=MESH)

    def l_copy(t_dp, t_in):
        return pltpu.make_async_remote_copy(
            src_ref=l_buf.at[me], dst_ref=l_buf.at[me], send_sem=ls_sem, recv_sem=l_sem.at[dp],
            device_id={"dp": t_dp, "inner": t_in}, device_id_type=MESH)

    def part_copy(r, t_in):
        rows = pl.ds(pl.multiple_of(r * rb + t_in * LQ, LQ), LQ)
        return pltpu.make_async_remote_copy(
            src_ref=part.at[rows, :], dst_ref=recv.at[me], send_sem=rs_sem, recv_sem=r_sem.at[dp],
            device_id={"dp": r, "inner": t_in}, device_id_type=MESH)

    def share(k, start):
        t_dp = lax.rem(dp + ndp - k, ndp)

        def one(i, _):
            t_in = lax.rem(inner + i, nin)
            q_copy(t_dp, t_in).start()
            l_copy(t_dp, t_in).start()
            return 0
        lax.fori_loop(start, nin, one, 0)
    share(0, 1)
    share(1, 0)

    gp_ref[...] = jnp.zeros_like(gp_ref)
    gacc[...] = jnp.zeros_like(gacc)
    d1[...] = jnp.zeros_like(d1)
    fetch.wait()
    for p in range(pages):
        p2[p, :, :dd] = p_ref[p]
        p2[p, :, dd:] = p_ref[p]
        pt[p] = p_ref[p].T
    share(2, 0)
    share(3, 0)

    def block(k):
        return lax.rem(dp + k, ndp)

    def arrived(k, r, count):
        qs, ls = q_buf.at[pl.ds(0, count * LQ), :], l_buf.at[pl.ds(0, count)]
        pltpu.make_async_copy(qs, qs, q_sem.at[r]).wait()
        pltpu.make_async_copy(ls, ls, l_sem.at[r]).wait()

    def split(r):
        for c in range(0, rb, 256):
            at = pl.ds(pl.multiple_of(r * rb + c, 256), 256)
            x = q_buf[at, :].astype(jnp.float32) * LOG2E
            hi = x.astype(jnp.bfloat16)
            q2[at, :dd] = hi
            q2[at, dd:] = (x - hi.astype(jnp.float32)).astype(jnp.bfloat16)

    def send(k):
        r = block(k)

        def one(i, _):
            t_in = lax.rem(inner + i, nin)

            @pl.when(i + k > 0)
            def _():
                part_copy(r, t_in).start()
            return 0
        lax.fori_loop(0, nin, one, 0)

    def units_a(r, p, s_ref, m_ref):
        at = pl.ds(pl.multiple_of(r * rb, rb), rb)

        def scores():
            s = lax.dot_general(p2[p], q2[at, :], (((1,), (1,)), ((), ())), preferred_element_type=jnp.float32)
            s_ref[...] = s
            m_ref[...] = jnp.max(s.reshape(lp // 8, 8, rb), axis=0)
        return [scores]

    def units_bc(r, p, s_ref, m_ref, d_ref):
        lane = lax.broadcasted_iota(jnp.int32, (8, 128), 1)
        st = {}
        b, c_ = [], []

        def start(h):
            m = m_ref[:, h:h + HW]
            m = jnp.broadcast_to(jnp.max(m, axis=0, keepdims=True), m.shape)
            st["m", h] = m
            st["l", h] = jnp.zeros((8, HW), jnp.float32)
            st["n", h] = jnp.zeros((8, HW), jnp.float32)

        def bt(h, k):
            if k == 0:
                start(h)
            y = s_ref[k:k + TR, h:h + HW].reshape(TR // 8, 8, HW)
            x = y - st["m", h][None]
            e = jnp.exp2(x)
            e0[k:k + TR, h:h + HW] = e.reshape(TR, HW)
            st["l", h] += jnp.sum(e, axis=0)
            st["n", h] += jnp.sum(e * x, axis=0)
            if k + TR == lp:
                finish(h)

        def finish(h):
            l = jnp.broadcast_to(jnp.sum(st["l", h], axis=0, keepdims=True), (8, HW))
            n = jnp.broadcast_to(jnp.sum(st["n", h], axis=0, keepdims=True), (8, HW))
            inv = 1.0 / l
            m2 = st["m", h] + n * inv
            tot = []
            for g in range(0, HW, 128):
                t = m2[:, g:g + 128]
                for w in (1, 2, 4, 8, 16):
                    up = pltpu.roll(t, 128 - w, 1)
                    dn = pltpu.roll(t, w, 1)
                    t = t + jnp.where((lane & w) == 0, up, dn)
                tot.append(t)
            score = jnp.concatenate(tot, axis=1) * LN2
            lab = []
            for g in range(0, HW, 128):
                rows = [jnp.broadcast_to(l_buf[r * (rb // LQ) + (h + g) // LQ + j], (8, 128)) for j in range(128 // LQ)]
                row = rows[-1]
                for j in range(128 // LQ - 2, -1, -1):
                    row = jnp.where(lane < (j + 1) * LQ, rows[j], row)
                lab.append(row)
            lab = jnp.concatenate(lab, axis=1)
            sign = jnp.where(lab == first + p, 1.0, -1.0).astype(jnp.float32)
            g = -sign / (1.0 + jnp.exp(sign * (score - float(LQ))))
            st["a", h] = g * inv * LN2
            st["c", h] = m2 - LOG2E

        def ct(h, k):
            y = s_ref[k:k + TR, h:h + HW].reshape(TR // 8, 8, HW)
            e = e0[k:k + TR, h:h + HW].reshape(TR // 8, 8, HW)
            d = (e * st["a", h][None]) * (y - st["c", h][None])
            d_ref[k:k + TR, h:h + HW] = d.reshape(TR, HW).astype(jnp.bfloat16)

        us = []
        for h in range(0, rb, HW):
            us += [functools.partial(bt, h, k) for k in range(0, lp, TR)]
        for h in range(0, rb, HW):
            us += [functools.partial(ct, h, k) for k in range(0, lp, TR)]
        return us

    def units_d(r, p, d_ref):
        at = pl.ds(pl.multiple_of(r * rb, rb), rb)

        def gq():
            t = jnp.dot(pt[p], d_ref[...], preferred_element_type=jnp.float32)
            if p == 0:
                gacc[...] = t
            elif p < pages - 1:
                gacc[...] += t
            else:
                part[at, :] = (gacc[...] + t).T.astype(part.dtype)

        def gp():
            gp_ref[p] += jnp.dot(d_ref[...], q_buf[at, :], preferred_element_type=jnp.float32)

        return [gq, gp]

    def weave(vec, mxu):
        n, k = len(vec), len(mxu)
        j = 0
        for i, u in enumerate(vec):
            while j < k and j * n <= i * k:
                mxu[j]()
                j += 1
            u()
        while j < k:
            mxu[j]()
            j += 1

    arrived(0, dp, nin - 1)
    split(dp)
    for u in units_a(dp, 0, s0, m0):
        u()

    def body(k, _):
        r = block(k)
        nxt = block(jnp.minimum(k + 1, nblk - 1))
        prev = block(jnp.maximum(k - 1, 0))

        @pl.when(k + 1 < nblk)
        def _():
            arrived(k + 1, nxt, nin)

        @pl.when(k + 4 < nblk)
        def _():
            share(k + 4, 0)
        split(nxt)
        for p in range(pages):
            nr = r if p + 1 < pages else nxt
            a = units_a(nr, (p + 1) % pages, sbuf[(p + 1) % 2], mbuf[(p + 1) % 2])
            bc = units_bc(r, p, sbuf[p % 2], mbuf[p % 2], dbuf[p % 2])
            d = units_d(r if p > 0 else prev, (p - 1) % pages, dbuf[(p - 1) % 2])
            weave(bc, d + a)

        @pl.when(k > 0)
        def _():
            send(k - 1)
        return 0

    lax.fori_loop(0, nblk, body, 0)
    last = block(nblk - 1)
    grad_q, grad_p = units_d(last, pages - 1, dbuf[(pages - 1) % 2])
    grad_q()
    recv[pl.ds(me, 1), :, :] = part[own, :][None]
    send(nblk - 1)
    grad_p()

    def landed(g, count):
        got = recv.at[pl.ds(0, count)]
        pltpu.make_async_copy(got, got, r_sem.at[g]).wait()

    def summed(g):
        terms = recv[pl.ds(pl.multiple_of(g * 16, 16), 16), :, :]
        return jnp.sum(terms.astype(jnp.float32), axis=0)

    landed(dp, nin - 1)
    for a in range(2, 8):
        landed(dps[a], nin)
    tot = summed(dp)
    for a in range(2, 8):
        tot += summed(dps[a])
    landed(dps[1], nin)
    out_ref[0] = tot + summed(dps[1])

    others = recv.at[pl.ds(0, total - 1)]
    pltpu.make_async_copy(others, others, rs_sem).wait()
    pltpu.make_async_copy(others, others, qs_sem).wait()
    labels = l_buf.at[pl.ds(0, total - 1)]
    pltpu.make_async_copy(labels, labels, ls_sem).wait()


def shards(queries, labels, pages):
    count, lp, dd = pages.shape
    total = lax.axis_size("dp") * lax.axis_size("inner")
    rows = total * LQ
    vm = pl.BlockSpec(memory_space=pltpu.VMEM)
    f32, bf16 = jnp.float32, jnp.bfloat16
    grad_pages, grad_queries = pl.pallas_call(
        step_kernel,
        out_shape=(jax.ShapeDtypeStruct(pages.shape, f32), jax.ShapeDtypeStruct(queries.shape, f32)),
        in_specs=[pl.BlockSpec(memory_space=pltpu.SMEM), vm, pl.BlockSpec(memory_space=pl.ANY)],
        out_specs=(vm, vm),
        scratch_shapes=[
            pltpu.VMEM((count, lp, dd), bf16),
            pltpu.VMEM((rows, dd), bf16),
            pltpu.VMEM((total, 1, 128), jnp.int32),
            pltpu.VMEM((rows, dd), bf16),
            pltpu.VMEM((total, LQ, dd), bf16),
            pltpu.VMEM((rows, 2 * dd), bf16),
            pltpu.VMEM((count, lp, 2 * dd), bf16),
            pltpu.VMEM((count, dd, lp), bf16),
            pltpu.VMEM((lp, RB), f32), pltpu.VMEM((lp, RB), f32),
            pltpu.VMEM((8, RB), f32), pltpu.VMEM((8, RB), f32),
            pltpu.VMEM((lp, RB), f32),
            pltpu.VMEM((lp, RB), bf16), pltpu.VMEM((lp, RB), bf16),
            pltpu.VMEM((dd, RB), f32),
            pltpu.SemaphoreType.DMA,
            pltpu.SemaphoreType.DMA((8,)),
            pltpu.SemaphoreType.DMA((8,)),
            pltpu.SemaphoreType.DMA((8,)),
            pltpu.SemaphoreType.DMA,
            pltpu.SemaphoreType.DMA,
            pltpu.SemaphoreType.DMA,
        ],
        compiler_params=pltpu.CompilerParams(vmem_limit_bytes=36 << 20, collective_id=0, has_side_effects=True),
        name="late_interaction",
    )(labels, queries, pages)
    return grad_queries, grad_pages


def solution(mesh):
    placed = (P(("dp", "inner"), None, None), P(("dp", "inner")), P(("dp", "inner"), None, None))
    return jax.shard_map(
        shards,
        mesh=mesh,
        in_specs=placed,
        out_specs=(P(("dp", "inner"), None, None), P(("dp", "inner"), None, None)),
        check_vma=False,
    )
```
